128 devices in a mesh: row: 32 (over y, x, core), col: 4 (over z).
Axes of the slice: x: 4, y: 4, z: 4, core: 2. Of those that a mesh axis runs over, the one named last changes fastest.
Arguments:
- velocity: float32 [512, 512, 2048], P(None, 'row', 'col'), may hold values from -6 to 6
- symbol_x: float32 [512], replicated, may hold values from 0.3 to 3
- symbol_y: float32 [512], replicated, may hold values from 0.3 to 3
- symbol_z: float32 [2048], replicated, may hold values from 0.3 to 3
Outputs:
- coefficients: float32 [512, 512, 2048], P('row', 'col')
The draws below stay inside these ranges and needn't reach their ends.
All inputs are finite; a program needn't handle non-finite values.
Results may differ from the reference program's by a relative error of at most 0.000076.
Values sent between devices are 32-bit elements; how exact they have to be, the bound alone decides.
A program may use at most 192 MiB of HBM per device.

```python
import jax
import jax.numpy as jnp
from jax import lax

GRID_X = 512
GRID_Y = 512
GRID_Z = 2048


def level_of(own_key, shape, pieces, low, largest):
    factor_of = 1.0
    for dim, shards_of in pieces:
        draws = jax.random.uniform(jax.random.fold_in(jax.random.fold_in(own_key, 6), dim), (shards_of,), jnp.float32, low / len(pieces), largest / len(pieces))
        factor_of = factor_of * jnp.repeat(jnp.exp(draws), shape[dim] // shards_of).reshape((-1,) + (1,) * (len(shape) - 1 - dim))
    return factor_of


def normal_values(stream_key, dims, width, limit, split=(), held_as=jnp.bfloat16):
    drawn = jax.random.normal(stream_key, dims, jnp.float32) * width
    if len(split) > 0:
        drawn = level_of(stream_key, dims, split, -0.22, 0.18) * drawn
    return jnp.clip(drawn, min=-limit, max=limit).astype(held_as)


def setup_inputs(seed: int = 0) -> dict:
    seeds = jax.random.split(jax.random.key(seed), 5)
    velocity = normal_values(seeds[0], (GRID_X, GRID_Y, GRID_Z), 1.0, 6.0, ((1, 32), (2, 4)), jnp.float32)
    symbol_x = jnp.clip(jax.random.uniform(seeds[1], (GRID_X,), jnp.float32, 0.3, 3.0), 0.3, 3.0)
    symbol_y = jnp.clip(jax.random.uniform(seeds[2], (GRID_Y,), jnp.float32, 0.3, 3.0), 0.3, 3.0)
    symbol_z = jnp.clip(jax.random.uniform(seeds[3], (GRID_Z,), jnp.float32, 0.3, 3.0), 0.3, 3.0)
    return {"velocity": velocity, "symbol_x": symbol_x, "symbol_y": symbol_y, "symbol_z": symbol_z}


def mode_table(count):
    rank = jnp.arange(count)
    angle = (2.0 * jnp.pi / count) * ((rank[:, None] * rank[None, :]) % count).astype(jnp.float32)
    return (jnp.cos(angle) + jnp.sin(angle)) * (count ** -0.5)


def along_dim(values, dim):
    moved = jnp.tensordot(values, mode_table(values.shape[dim]), axes=([dim], [0]), precision=lax.Precision.HIGHEST)
    return jnp.moveaxis(moved, -1, dim)


def reference(velocity, symbol_x, symbol_y, symbol_z):
    coefficients = velocity
    coefficients = along_dim(coefficients, 0)
    coefficients = along_dim(coefficients, 1)
    coefficients = along_dim(coefficients, 2)
    symbol = symbol_x[:, None, None] + symbol_y[None, :, None] + symbol_z[None, None, :]
    coefficients = coefficients * ((1.0 - 0.2 * symbol) / (1.0 + 0.2 * symbol))
    return coefficients
```

```python
import functools

import jax
import jax.numpy as jnp
import numpy as np
from jax import lax
from jax.experimental import pallas as pl
from jax.experimental.pallas import tpu as pltpu
from jax.sharding import PartitionSpec as P

MESH = pl.DeviceIdType.MESH
F32 = jnp.float32
BF16 = jnp.bfloat16
FINE = 32


def split(values):
    head = values.astype(BF16)
    return head, (values - head.astype(F32)).astype(BF16)


def mode_table(count):
    rank = np.arange(count)
    angle = 2.0 * np.pi / count * (rank[:, None] * rank[None, :] % count)
    return ((np.cos(angle) + np.sin(angle)) / np.sqrt(count)).astype(np.float32)


def stacked_table(count):
    table = mode_table(count)
    head = table.astype(BF16)
    rest = (table - head.astype(np.float32)).astype(BF16)
    return np.concatenate([head, rest, head], axis=1)


def factor_tables(count):
    k = np.arange(count)
    coarse = 2.0 * np.pi / count * (FINE * np.arange(count // FINE)[:, None] * k % count)
    fine = 2.0 * np.pi / count * (np.arange(FINE)[:, None] * k % count)
    scale = 1.0 / np.sqrt(count)
    tables = np.cos(coarse), np.sin(coarse), (np.cos(fine) + np.sin(fine)) * scale, (np.cos(fine) - np.sin(fine)) * scale
    return [t.astype(np.float32) for t in tables]


def x_kernel(v_ref, h_ref, o_ref, parts):
    nx, ny, lanes = v_ref.shape
    v = v_ref.reshape(nx * ny, lanes)
    o = o_ref.reshape(nx * ny, lanes)
    for y in range(ny):
        head, rest = split(v[pl.ds(y, nx, stride=ny), :])
        at = pl.ds(y * lanes, lanes)
        parts[0:nx, at] = head
        parts[nx : 2 * nx, at] = head
        parts[2 * nx : 3 * nx, at] = rest
    for y in range(0, ny, 2):
        made = jnp.dot(h_ref[...], parts[:, y * lanes : (y + 2) * lanes], preferred_element_type=F32)
        o[pl.ds(y, nx, stride=ny), :] = made[:, :lanes]
        o[pl.ds(y + 1, nx, stride=ny), :] = made[:, lanes:]


def x_transform(velocity, table):
    nx, ny, nz = velocity.shape
    block = pl.BlockSpec((nx, 8, 128), lambda y, z: (0, y, z))
    return pl.pallas_call(
        x_kernel,
        grid=(ny // 8, nz // 128),
        in_specs=[block, pl.BlockSpec(table.shape, lambda y, z: (0, 0))],
        out_specs=block,
        out_shape=jax.ShapeDtypeStruct(velocity.shape, F32),
        scratch_shapes=[pltpu.VMEM((3 * nx, 8 * 128), BF16)],
        compiler_params=pltpu.CompilerParams(vmem_limit_bytes=40 * 2**20),
    )(velocity, table)


def exchange_kernel(
    rows, cols, sent, h_ref, cos_ref, sin_ref, plus_ref, minus_ref, out,
    got_y, got_z, t_head, t_rest, made_y, made_z, parts_y, parts_z,
    row_send, row_recv, own_sem, col_send, col_recv, out_sem,
):
    chunks, ny, zs = got_y.shape
    ys, nz = got_z.shape[1:]
    yl = ny // rows
    row, col = lax.axis_index("row"), lax.axis_index("col")

    barrier = pltpu.get_barrier_semaphore()

    @pl.loop(1, rows)
    def _(o):
        pl.semaphore_signal(barrier, inc=1, device_id={"row": lax.rem(row + o, rows)}, device_id_type=MESH)

    for d in range(1, cols):
        pl.semaphore_signal(barrier, inc=1, device_id={"col": lax.rem(col + d, cols)}, device_id_type=MESH)
    pl.semaphore_wait(barrier, rows + cols - 2)

    mine = pl.ds(pl.multiple_of(row * yl, yl), yl)

    @pl.loop(0, chunks)
    def _(j):
        @pl.loop(1, rows)
        def _(o):
            y = lax.rem(row // 8 + o // 8, 4)
            x = lax.rem(row // 2 + o // 2, 4)
            c = lax.rem(row + o, 2)
            p = y * 8 + x * 2 + c
            pltpu.make_async_remote_copy(
                src_ref=sent.at[p * chunks + j], dst_ref=got_y.at[j, mine],
                send_sem=row_send, recv_sem=row_recv.at[j], device_id={"row": p}, device_id_type=MESH,
            ).start()

        pltpu.make_async_copy(sent.at[row * chunks + j], got_y.at[j, mine], own_sem.at[j]).start()

    @pl.loop(0, nz // FINE)
    def _(i):
        table = cos_ref[pl.ds(i, 1), :] * plus_ref[...] + sin_ref[pl.ds(i, 1), :] * minus_ref[...]
        head, rest = split(table)
        at = pl.ds(pl.multiple_of(i * FINE, FINE), FINE)
        t_head[at, :] = head
        t_rest[at, :] = rest

    def col_sends(j, slot):
        return [
            pltpu.make_async_remote_copy(
                src_ref=made_y.at[slot, pl.ds(pl.multiple_of(q * ys, ys), ys)],
                dst_ref=got_z.at[j, :, pl.ds(pl.multiple_of(col * zs, zs), zs)],
                send_sem=col_send.at[slot], recv_sem=col_recv.at[j], device_id={"col": q}, device_id_type=MESH,
            )
            for q in [lax.rem(col + d, cols) for d in (1, 3, 2)]
        ]

    def wait_sends(slot):
        sends = made_y.at[slot, pl.ds(0, (cols - 1) * ys)]
        pltpu.make_async_copy(sends, sends, col_send.at[slot]).wait()

    def wait_out(j, slot):
        pltpu.make_async_copy(made_z.at[slot], out.at[j], out_sem.at[slot]).wait()

    def y_step(j):
        slot = lax.rem(j, 2)
        pltpu.make_async_copy(sent.at[row * chunks + j], got_y.at[j, mine], own_sem.at[j]).wait()
        landed = got_y.at[j, pl.ds(0, (rows - 1) * yl)]
        pltpu.make_async_copy(landed, landed, row_recv.at[j]).wait()
        head, rest = split(got_y[j])
        parts_y[0:ny, :] = head
        parts_y[ny : 2 * ny, :] = head
        parts_y[2 * ny : 3 * ny, :] = rest

        @pl.when(j >= 2)
        def _():
            wait_sends(slot)

        @pl.loop(0, zs // 256)
        def _(n):
            at = pl.ds(pl.multiple_of(n * 256, 256), 256)
            made_y[slot, :, at] = jnp.dot(h_ref[...], parts_y[:, at], preferred_element_type=F32)

        got_z[j, :, pl.ds(pl.multiple_of(col * zs, zs), zs)] = made_y[slot, pl.ds(pl.multiple_of(col * ys, ys), ys), :]
        for copy in col_sends(j, slot):
            copy.start()

    def z_step(j):
        slot = lax.rem(j, 2)
        landed = got_z.at[j, :, pl.ds(0, (cols - 1) * zs)]
        pltpu.make_async_copy(landed, landed, col_recv.at[j]).wait()
        head, rest = split(got_z[j])
        parts_z[0:ys, :] = head
        parts_z[ys : 2 * ys, :] = rest

        @pl.when(j >= 2)
        def _():
            wait_out(j - 2, slot)

        @pl.loop(0, nz // 512)
        def _(n):
            at = pl.ds(pl.multiple_of(n * 512, 512), 512)
            both = jnp.dot(parts_z[...], t_head[:, at], preferred_element_type=F32)
            small = jnp.dot(parts_z[0:ys, :], t_rest[:, at], preferred_element_type=F32)
            made_z[slot, :, at] = both[:ys] + (both[ys:] + small)

        pltpu.make_async_copy(made_z.at[slot], out.at[j], out_sem.at[slot]).start()

    @pl.loop(0, chunks + 1)
    def _(t):
        @pl.when(t < chunks)
        def _():
            y_step(t)

        @pl.when(t >= 1)
        def _():
            z_step(t - 1)

    for slot in range(2):
        wait_sends(slot)
        wait_out(chunks - 2 + slot, slot)
    gone = sent.at[pl.ds(0, (rows - 1) * chunks)]
    pltpu.make_async_copy(gone, gone, row_send).wait()


def exchange(sent, table, factors, rows, cols):
    nx, yl, zs = sent.shape
    chunks, ny, nz = nx // rows, yl * rows, zs * cols
    ys = ny // cols
    anywhere = pl.BlockSpec(memory_space=pl.ANY)
    vmem = pl.BlockSpec(memory_space=pltpu.VMEM)
    dma = pltpu.SemaphoreType.DMA
    return pl.pallas_call(
        functools.partial(exchange_kernel, rows, cols),
        in_specs=[anywhere] + [vmem] * 5,
        out_specs=anywhere,
        out_shape=jax.ShapeDtypeStruct((chunks, ys, nz), F32),
        scratch_shapes=[
            pltpu.VMEM((chunks, ny, zs), F32),
            pltpu.VMEM((chunks, ys, nz), F32),
            pltpu.VMEM((nz, nz), BF16),
            pltpu.VMEM((nz, nz), BF16),
            pltpu.VMEM((2, ny, zs), F32),
            pltpu.VMEM((2, ys, nz), F32),
            pltpu.VMEM((3 * ny, zs), BF16),
            pltpu.VMEM((2 * ys, nz), BF16),
            dma, dma((chunks,)), dma((chunks,)), dma((2,)), dma((chunks,)), dma((2,)),
        ],
        compiler_params=pltpu.CompilerParams(collective_id=0, has_side_effects=True, vmem_limit_bytes=67043328),
    )(sent, table, *factors)


def solution(mesh):
    rows, cols = mesh.shape["row"], mesh.shape["col"]

    def local(velocity, symbol_x, symbol_y, symbol_z):
        table = jnp.asarray(stacked_table(velocity.shape[0]))
        factors = [jnp.asarray(t) for t in factor_tables(velocity.shape[2] * cols)]
        values = x_transform(velocity, table)
        values = exchange(values, table, factors, rows, cols)
        share_x, share_y = values.shape[:2]
        part_x = lax.dynamic_slice_in_dim(symbol_x, lax.axis_index("row") * share_x, share_x)
        part_y = lax.dynamic_slice_in_dim(symbol_y, lax.axis_index("col") * share_y, share_y)
        symbol = part_x[:, None, None] + part_y[None, :, None] + symbol_z[None, None, :]
        return values * ((1.0 - 0.2 * symbol) / (1.0 + 0.2 * symbol))

    placed = (P(None, "row", "col"), P(), P(), P())
    return jax.shard_map(local, mesh=mesh, in_specs=placed, out_specs=P("row", "col", None), check_vma=False)
```

```python
import functools

import jax
import jax.numpy as jnp
import numpy as np
from jax import lax
from jax.experimental import pallas as pl
from jax.experimental.pallas import tpu as pltpu
from jax.sharding import PartitionSpec as P

MESH = pl.DeviceIdType.MESH
F32 = jnp.float32
BF16 = jnp.bfloat16
FINE = 32
LANES = 128
Y_BLOCK = 8
AHEAD = 4
Y_LAG = 3
SLOTS = 4


def split(values):
    head = values.astype(BF16)
    return head, (values - head.astype(F32)).astype(BF16)


def mode_table(count):
    rank = np.arange(count)
    angle = 2.0 * np.pi / count * (rank[:, None] * rank[None, :] % count)
    return ((np.cos(angle) + np.sin(angle)) / np.sqrt(count)).astype(np.float32)


def stacked_table(count):
    table = mode_table(count)
    head = table.astype(BF16)
    rest = (table - head.astype(np.float32)).astype(BF16)
    return np.concatenate([head, rest, head], axis=1)


def factor_tables(count):
    k = np.arange(count)
    coarse = 2.0 * np.pi / count * (FINE * np.arange(count // 2 // FINE)[:, None] * k % count)
    fine = 2.0 * np.pi / count * (np.arange(FINE)[:, None] * k % count)
    scale = 1.0 / np.sqrt(count)
    tables = np.cos(coarse), np.sin(coarse), (np.cos(fine) + np.sin(fine)) * scale, (np.cos(fine) - np.sin(fine)) * scale
    return [t.astype(np.float32) for t in tables]


def kernel(
    rows, cols, velocity, h_ref, cos_ref, sin_ref, plus_ref, minus_ref, sx_ref, sy_ref, sz_ref, out, sent,
    v_in, v_out, parts_x, got_y, got_z, t_head, t_rest, made_y, made_z, parts_y, parts_z, sy_col,
    in_sem, keep_sem, row_send, row_recv, own_sem, col_send, col_recv, out_sem,
):
    nx, yl, zs = velocity.shape
    chunks, ys, nz = out.shape
    ny = yl * rows
    quarters = zs // LANES
    units = chunks * quarters
    halves = yl // Y_BLOCK
    blocks = quarters * halves
    early = blocks
    row, col = lax.axis_index("row"), lax.axis_index("col")
    mine = pl.ds(pl.multiple_of(row * yl, yl), yl)

    def place(u):
        first = lax.div(units + early - 1 - u, units)
        j = first * lax.rem(u, 2) + (1 - first) * lax.div(u, quarters)
        q = first * lax.div(u, 2) + (1 - first) * lax.rem(u, quarters)
        return j, q

    def block_of(ref, b):
        y, z = lax.rem(b, halves), lax.div(b, halves)
        return ref.at[:, pl.ds(pl.multiple_of(y * Y_BLOCK, Y_BLOCK), Y_BLOCK), pl.ds(pl.multiple_of(z * LANES, LANES), LANES)]

    def kept_at(b):
        y, z = lax.rem(b, halves), lax.div(b, halves)
        return sent.at[z, :, pl.ds(pl.multiple_of(y * Y_BLOCK, Y_BLOCK), Y_BLOCK), :]

    def load(b):
        slot = lax.rem(b, 2)
        return pltpu.make_async_copy(block_of(velocity, b), v_in.at[slot], in_sem.at[slot])

    def keep(b):
        slot = lax.rem(b, 2)
        return pltpu.make_async_copy(v_out.at[slot], kept_at(b), keep_sem.at[slot])

    def x_step(b):
        slot = lax.rem(b, 2)
        load(b).wait()
        v = v_in.at[slot].reshape(nx * Y_BLOCK, LANES)
        o = v_out.at[slot].reshape(nx * Y_BLOCK, LANES)
        for y in range(0, Y_BLOCK, 2):
            for n in (y, y + 1):
                head, rest = split(v[pl.ds(n, nx, stride=Y_BLOCK), :])
                at = pl.ds(n * LANES, LANES)
                parts_x[0:nx, at] = head
                parts_x[nx : 2 * nx, at] = head
                parts_x[2 * nx : 3 * nx, at] = rest
            made = jnp.dot(h_ref[...], parts_x[:, y * LANES : (y + 2) * LANES], preferred_element_type=F32)
            o[pl.ds(y, nx, stride=Y_BLOCK), :] = made[:, :LANES]
            o[pl.ds(y + 1, nx, stride=Y_BLOCK), :] = made[:, LANES:]
        keep(b).start()

        @pl.when(b + 2 < blocks)
        def _():
            load(b + 2).start()

    def own(u):
        j, q = place(u)
        return pltpu.make_async_copy(sent.at[q, row * chunks + j], got_y.at[u, mine], own_sem.at[u])

    def row_sends(u):
        j, q = place(u)

        @pl.loop(1, rows)
        def _(o):
            y = lax.rem(lax.div(row, 8) + lax.div(o, 8), 4)
            x = lax.rem(lax.div(row, 2) + lax.div(o, 2), 4)
            c = lax.rem(row + o, 2)
            p = y * 8 + x * 2 + c
            pltpu.make_async_remote_copy(
                src_ref=sent.at[q, p * chunks + j], dst_ref=got_y.at[u, mine],
                send_sem=row_send, recv_sem=row_recv.at[u], device_id={"row": p}, device_id_type=MESH,
            ).start()

        own(u).start()

    def wait_sends(slot):
        sends = made_y.at[slot, pl.ds(0, (cols - 1) * ys)]
        pltpu.make_async_copy(sends, sends, col_send.at[slot]).wait()

    def y_step(u):
        slot = lax.rem(u, SLOTS)
        j, q = place(u)
        own(u).wait()
        landed = got_y.at[u, pl.ds(0, (rows - 1) * yl)]
        pltpu.make_async_copy(landed, landed, row_recv.at[u]).wait()
        head, rest = split(got_y[u])
        parts_y[0:ny, :] = head
        parts_y[ny : 2 * ny, :] = head
        parts_y[2 * ny : 3 * ny, :] = rest

        @pl.when(u >= SLOTS)
        def _():
            wait_sends(slot)

        made_y[slot] = jnp.dot(h_ref[...], parts_y[...], preferred_element_type=F32)
        to = got_z.at[j, col * quarters + q]
        to[...] = made_y[slot, pl.ds(pl.multiple_of(col * ys, ys), ys), :]
        for d in (1, 3, 2):
            p = lax.rem(col + d, cols)
            pltpu.make_async_remote_copy(
                src_ref=made_y.at[slot, pl.ds(pl.multiple_of(p * ys, ys), ys)], dst_ref=to,
                send_sem=col_send.at[slot], recv_sem=col_recv.at[j], device_id={"col": p}, device_id_type=MESH,
            ).start()

    def wait_out(j, slot):
        pltpu.make_async_copy(made_z.at[slot], out.at[j], out_sem.at[slot]).wait()

    def z_step(j):
        slot = lax.rem(j, 2)
        landed = got_z.at[j, pl.ds(0, (cols - 1) * quarters)]
        pltpu.make_async_copy(landed, landed, col_recv.at[j]).wait()
        fold = cols * quarters // 2
        for k in range(fold):
            low, high = got_z[j, k], got_z[j, k + fold]
            at = pl.ds(k * LANES, LANES)
            for n, value in enumerate((low + high, low - high)):
                head, rest = split(value)
                parts_z[n * ys : (n + 1) * ys, at] = head
                parts_z[(n + 2) * ys : (n + 3) * ys, at] = rest

        @pl.when(j >= 2)
        def _():
            wait_out(j - 2, slot)

        part = sx_ref[row * chunks + j] + sy_col[...]
        even = lax.rem(lax.broadcasted_iota(jnp.int32, (ys, LANES), 1), 2) == 0

        @pl.loop(0, nz // 512)
        def _(n):
            at = pl.ds(pl.multiple_of(n * 512, 512), 512)
            both = jnp.dot(parts_z[...], t_head[:, at], preferred_element_type=F32)
            small = jnp.dot(parts_z[0 : 2 * ys, :], t_rest[:, at], preferred_element_type=F32)
            total = both[: 2 * ys] + (both[2 * ys :] + small)
            for m in range(512 // LANES):
                lanes = slice(m * LANES, (m + 1) * LANES)
                value = jnp.where(even, total[:ys, lanes], total[ys:, lanes])
                to = pl.ds(pl.multiple_of(n * 512 + m * LANES, LANES), LANES)
                symbol = part + sz_ref[:, to]
                made_z[slot, :, to] = value * ((1.0 - 0.2 * symbol) / (1.0 + 0.2 * symbol))

        pltpu.make_async_copy(made_z.at[slot], out.at[j], out_sem.at[slot]).start()

    load(0).start()
    load(1).start()
    barrier = pltpu.get_barrier_semaphore()

    @pl.loop(1, rows)
    def _(o):
        pl.semaphore_signal(barrier, inc=1, device_id={"row": lax.rem(row + o, rows)}, device_id_type=MESH)

    for d in range(1, cols):
        pl.semaphore_signal(barrier, inc=1, device_id={"col": lax.rem(col + d, cols)}, device_id_type=MESH)

    @pl.loop(0, halves)
    def _(t):
        x_step(t)

    pl.semaphore_wait(barrier, rows + cols - 2)

    @pl.loop(halves - 1, 4 * chunks + 9)
    def _(t):
        @pl.when(jnp.logical_and(t >= halves, t < blocks))
        def _():
            x_step(t)

        @pl.when(t < blocks)
        def _():
            @pl.when(lax.rem(t, halves) == halves - 1)
            def _():
                for h in range(halves):
                    keep(t - (halves - 1) + h).wait()

                @pl.loop(t - 1, t + 1)
                def _(u):
                    row_sends(u)

        @pl.when(t == blocks)
        def _():
            @pl.loop(0, nz // 2 // FINE)
            def _(i):
                table = cos_ref[pl.ds(i, 1), :] * plus_ref[...] + sin_ref[pl.ds(i, 1), :] * minus_ref[...]
                head, rest = split(table)
                at = pl.ds(pl.multiple_of(i * FINE, FINE), FINE)
                t_head[at, :] = head
                t_rest[at, :] = rest

            spread = jnp.broadcast_to(sy_ref[:, pl.ds(pl.multiple_of(col * ys, ys), ys)], (LANES, ys))
            sy_col[...] = spread.T

        @pl.when(jnp.logical_and(t >= blocks - 1, t < units - AHEAD))
        def _():
            late = lax.div(units + blocks - 1 - t, units)

            @pl.loop(t + AHEAD - late * (AHEAD - 1), t + AHEAD + 1)
            def _(u):
                row_sends(u)

        @pl.when(jnp.logical_and(t >= Y_LAG, t < units + Y_LAG))
        def _():
            y_step(t - Y_LAG)

        @pl.when(jnp.logical_and(t >= 12, lax.rem(t, 4) == 0))
        def _():
            z_step(lax.div(t, 4) - 3)

    for slot in range(SLOTS):
        wait_sends(slot)
    for slot in range(2):
        wait_out(chunks - 2 + slot, slot)
    gone = sent.at[:, pl.ds(0, (rows - 1) * chunks)]
    pltpu.make_async_copy(gone, gone, row_send).wait()


def solution(mesh):
    rows, cols = mesh.shape["row"], mesh.shape["col"]

    def local(velocity, symbol_x, symbol_y, symbol_z):
        nx, yl, zs = velocity.shape
        chunks, ny, nz = nx // rows, yl * rows, zs * cols
        ys, quarters = ny // cols, zs // LANES
        units = chunks * quarters
        table = jnp.asarray(stacked_table(nx))
        factors = [jnp.asarray(t) for t in factor_tables(nz)]
        anywhere = pl.BlockSpec(memory_space=pl.ANY)
        vmem = pl.BlockSpec(memory_space=pltpu.VMEM)
        dma = pltpu.SemaphoreType.DMA
        out, _ = pl.pallas_call(
            functools.partial(kernel, rows, cols),
            in_specs=[anywhere] + [vmem] * 5 + [pl.BlockSpec(memory_space=pltpu.SMEM), vmem, vmem],
            out_specs=(anywhere, anywhere),
            out_shape=(
                jax.ShapeDtypeStruct((chunks, ys, nz), F32),
                jax.ShapeDtypeStruct((quarters, nx, yl, LANES), F32),
            ),
            scratch_shapes=[
                pltpu.VMEM((2, nx, Y_BLOCK, LANES), F32),
                pltpu.VMEM((2, nx, Y_BLOCK, LANES), F32),
                pltpu.VMEM((3 * nx, Y_BLOCK * LANES), BF16),
                pltpu.VMEM((units, ny, LANES), F32),
                pltpu.VMEM((chunks, nz // LANES, ys, LANES), F32),
                pltpu.VMEM((nz // 2, nz), BF16),
                pltpu.VMEM((nz // 2, nz), BF16),
                pltpu.VMEM((SLOTS, ny, LANES), F32),
                pltpu.VMEM((2, ys, nz), F32),
                pltpu.VMEM((3 * ny, LANES), BF16),
                pltpu.VMEM((4 * ys, nz // 2), BF16),
                pltpu.VMEM((ys, LANES), F32),
                dma((2,)), dma((2,)), dma, dma((units,)), dma((units,)), dma((SLOTS,)), dma((chunks,)), dma((2,)),
            ],
            compiler_params=pltpu.CompilerParams(collective_id=0, has_side_effects=True, vmem_limit_bytes=67043328),
        )(velocity, table, *factors, symbol_x, symbol_y[None, :], symbol_z[None, :])
        return out

    placed = (P(None, "row", "col"), P(), P(), P())
    return jax.shard_map(local, mesh=mesh, in_specs=placed, out_specs=P("row", "col", None), check_vma=False)
```

```python
import functools

import jax
import jax.numpy as jnp
import numpy as np
from jax import lax
from jax.experimental import pallas as pl
from jax.experimental.pallas import tpu as pltpu
from jax.sharding import PartitionSpec as P

MESH = pl.DeviceIdType.MESH
F32 = jnp.float32
BF16 = jnp.bfloat16
FINE = 32
LANES = 128
Y_BLOCK = 8
AHEAD = 4
Y_LAG = 3
SLOTS = 4


def split(values):
    head = values.astype(BF16)
    return head, (values - head.astype(F32)).astype(BF16)


def mode_table(count):
    rank = np.arange(count)
    angle = 2.0 * np.pi / count * (rank[:, None] * rank[None, :] % count)
    return ((np.cos(angle) + np.sin(angle)) / np.sqrt(count)).astype(np.float32)


def stacked_table(count):
    table = mode_table(count)
    head = table.astype(BF16)
    rest = (table - head.astype(np.float32)).astype(BF16)
    return np.concatenate([head, rest, head], axis=1)


def factor_tables(count):
    k = np.arange(count)
    coarse = 2.0 * np.pi / count * (FINE * np.arange(count // 2 // FINE)[:, None] * k % count)
    fine = 2.0 * np.pi / count * (np.arange(FINE)[:, None] * k % count)
    scale = 1.0 / np.sqrt(count)
    tables = np.cos(coarse), np.sin(coarse), (np.cos(fine) + np.sin(fine)) * scale, (np.cos(fine) - np.sin(fine)) * scale
    return [t.astype(np.float32) for t in tables]


def kernel(
    rows, cols, velocity, h_ref, cos_ref, sin_ref, plus_ref, minus_ref, sx_ref, sy_ref, sz_ref, out, sent,
    got_y, got_z, t_head, t_rest, made_y, parts_y, parts_z, sy_col,
    in_sem, keep_sem, row_send, row_recv, own_sem, col_send, col_recv, free_sem,
):
    nx, yl, zs = velocity.shape
    chunks, ys, nz = out.shape
    ny = yl * rows
    quarters = zs // LANES
    units = chunks * quarters
    halves = yl // Y_BLOCK
    blocks = quarters * halves
    early = blocks
    row, col = lax.axis_index("row"), lax.axis_index("col")
    mine = pl.ds(pl.multiple_of(row * yl, yl), yl)

    ring_y = [lax.rem(lax.div(row, 8) + d, 4) * 8 for d in range(4)]
    ring_x = [lax.rem(lax.div(row, 2) + d, 4) * 2 for d in range(4)]
    pair = [lax.rem(row + d, 2) for d in range(2)]
    peers = [ring_y[o // 8] + ring_x[o // 2 % 4] + pair[o % 2] for o in range(1, rows)]

    def place(u):
        first = lax.div(units + early - 1 - u, units)
        j = first * lax.rem(u, 2) + (1 - first) * lax.div(u, quarters)
        q = first * lax.div(u, 2) + (1 - first) * lax.rem(u, quarters)
        return j, q

    def block_of(ref, b):
        y, z = lax.rem(b, halves), lax.div(b, halves)
        return ref.at[:, pl.ds(pl.multiple_of(y * Y_BLOCK, Y_BLOCK), Y_BLOCK), pl.ds(pl.multiple_of(z * LANES, LANES), LANES)]

    def kept_at(b):
        y, z = lax.rem(b, halves), lax.div(b, halves)
        return sent.at[z, :, pl.ds(pl.multiple_of(y * Y_BLOCK, Y_BLOCK), Y_BLOCK), :]

    late = chunks // 2
    tiles = got_z.reshape(chunks * nz * ys // LANES // Y_BLOCK, Y_BLOCK, LANES)
    lines = got_z.reshape(chunks * nz * ys // LANES, LANES)
    base = late * nz * ys // LANES // Y_BLOCK

    def load(b):
        slot = lax.rem(b, 2)
        at = pl.ds(base + slot * nx, nx)
        return pltpu.make_async_copy(block_of(velocity, b), tiles.at[at], in_sem.at[slot])

    def keep(b):
        slot = lax.rem(b, 2)
        at = pl.ds(base + (2 + slot) * nx, nx)
        return pltpu.make_async_copy(tiles.at[at], kept_at(b), keep_sem.at[slot])

    def x_step(b):
        slot = lax.rem(b, 2)
        load(b).wait()
        v = lines.at[pl.ds(pl.multiple_of((base + slot * nx) * Y_BLOCK, Y_BLOCK), nx * Y_BLOCK)]
        o = lines.at[pl.ds(pl.multiple_of((base + (2 + slot) * nx) * Y_BLOCK, Y_BLOCK), nx * Y_BLOCK)]
        for y in range(0, Y_BLOCK, 2):
            for n in (y, y + 1):
                head, rest = split(v[pl.ds(n, nx, stride=Y_BLOCK), :])
                at = pl.ds(n * LANES, LANES)
                t_head[0:nx, at] = head
                t_head[nx : 2 * nx, at] = head
                t_rest[0:nx, at] = rest
            lanes = slice(y * LANES, (y + 2) * LANES)
            made = jnp.dot(h_ref[:, : 2 * nx], t_head[0 : 2 * nx, lanes], preferred_element_type=F32)
            made += jnp.dot(h_ref[:, 2 * nx :], t_rest[0:nx, lanes], preferred_element_type=F32)
            o[pl.ds(y, nx, stride=Y_BLOCK), :] = made[:, :LANES]
            o[pl.ds(y + 1, nx, stride=Y_BLOCK), :] = made[:, LANES:]
        keep(b).start()

        @pl.when(b + 2 < blocks)
        def _():
            load(b + 2).start()

    def own(u):
        j, q = place(u)
        return pltpu.make_async_copy(sent.at[q, row * chunks + j], got_y.at[u, mine], own_sem.at[u])

    def row_sends(u):
        j, q = place(u)

        to = got_y.at[u, mine]
        for p in peers:
            pltpu.make_async_remote_copy(
                src_ref=sent.at[q, p * chunks + j], dst_ref=to,
                send_sem=row_send, recv_sem=row_recv.at[u], device_id={"row": p}, device_id_type=MESH,
            ).start()

        own(u).start()

    def wait_sends(slot):
        sends = made_y.at[slot, pl.ds(0, (cols - 1) * ys)]
        pltpu.make_async_copy(sends, sends, col_send.at[slot]).wait()

    def y_step(u):
        slot = lax.rem(u, SLOTS)
        j, q = place(u)
        own(u).wait()
        landed = got_y.at[u, pl.ds(0, (rows - 1) * yl)]
        pltpu.make_async_copy(landed, landed, row_recv.at[u]).wait()
        head, rest = split(got_y[u])
        parts_y[0:ny, :] = head
        parts_y[ny : 2 * ny, :] = head
        parts_y[2 * ny : 3 * ny, :] = rest

        @pl.when(u >= SLOTS)
        def _():
            wait_sends(slot)

        @pl.when(u == late * quarters)
        def _():
            pl.semaphore_wait(free_sem, cols - 1)

        made_y[slot] = jnp.dot(h_ref[...], parts_y[...], preferred_element_type=F32)
        to = got_z.at[j, col * quarters + q]
        to[...] = made_y[slot, pl.ds(pl.multiple_of(col * ys, ys), ys), :]
        for d in (1, 3, 2):
            p = lax.rem(col + d, cols)
            pltpu.make_async_remote_copy(
                src_ref=made_y.at[slot, pl.ds(pl.multiple_of(p * ys, ys), ys)], dst_ref=to,
                send_sem=col_send.at[slot], recv_sem=col_recv.at[j], device_id={"col": p}, device_id_type=MESH,
            ).start()

    def z_step(j):
        landed = got_z.at[j, pl.ds(0, (cols - 1) * quarters)]
        pltpu.make_async_copy(landed, landed, col_recv.at[j]).wait()
        fold = cols * quarters // 2
        for k in range(fold):
            low, high = got_z[j, k], got_z[j, k + fold]
            at = pl.ds(k * LANES, LANES)
            for n, value in enumerate((low + high, low - high)):
                head, rest = split(value)
                parts_z[n * ys : (n + 1) * ys, at] = head
                parts_z[(n + 2) * ys : (n + 3) * ys, at] = rest

        part = sx_ref[row * chunks + j] + sy_col[...]
        even = lax.rem(lax.broadcasted_iota(jnp.int32, (ys, LANES), 1), 2) == 0

        @pl.loop(0, nz // 512)
        def _(n):
            at = pl.ds(pl.multiple_of(n * 512, 512), 512)
            both = jnp.dot(parts_z[...], t_head[:, at], preferred_element_type=F32)
            small = jnp.dot(parts_z[0 : 2 * ys, :], t_rest[:, at], preferred_element_type=F32)
            total = both[: 2 * ys] + (both[2 * ys :] + small)
            for m in range(512 // LANES):
                lanes = slice(m * LANES, (m + 1) * LANES)
                value = jnp.where(even, total[:ys, lanes], total[ys:, lanes])
                to = pl.ds(pl.multiple_of(n * 512 + m * LANES, LANES), LANES)
                symbol = part + sz_ref[:, to]
                out[j, :, to] = value * ((1.0 - 0.2 * symbol) / (1.0 + 0.2 * symbol))

    load(0).start()
    load(1).start()
    barrier = pltpu.get_barrier_semaphore()

    @pl.loop(1, rows)
    def _(o):
        pl.semaphore_signal(barrier, inc=1, device_id={"row": lax.rem(row + o, rows)}, device_id_type=MESH)

    for d in range(1, cols):
        pl.semaphore_signal(barrier, inc=1, device_id={"col": lax.rem(col + d, cols)}, device_id_type=MESH)

    @pl.loop(0, halves)
    def _(t):
        x_step(t)

    pl.semaphore_wait(barrier, rows + cols - 2)

    @pl.loop(halves - 1, 4 * chunks + 9)
    def _(t):
        @pl.when(jnp.logical_and(t >= halves, t < blocks))
        def _():
            x_step(t)

        @pl.when(t < blocks)
        def _():
            @pl.when(lax.rem(t, halves) == halves - 1)
            def _():
                for h in range(halves):
                    keep(t - (halves - 1) + h).wait()

                @pl.loop(t - 1, t + 1)
                def _(u):
                    row_sends(u)

                @pl.when(t == blocks - 1)
                def _():
                    for d in range(1, cols):
                        p = lax.rem(col + d, cols)
                        pl.semaphore_signal(free_sem, inc=1, device_id={"col": p}, device_id_type=MESH)

        @pl.when(t == blocks)
        def _():
            @pl.loop(0, nz // 2 // FINE)
            def _(i):
                table = cos_ref[pl.ds(i, 1), :] * plus_ref[...] + sin_ref[pl.ds(i, 1), :] * minus_ref[...]
                head, rest = split(table)
                at = pl.ds(pl.multiple_of(i * FINE, FINE), FINE)
                t_head[at, :] = head
                t_rest[at, :] = rest

            spread = jnp.broadcast_to(sy_ref[:, pl.ds(pl.multiple_of(col * ys, ys), ys)], (LANES, ys))
            sy_col[...] = spread.T

        @pl.when(jnp.logical_and(t >= blocks - 1, t < units - AHEAD))
        def _():
            last = lax.div(units + blocks - 1 - t, units)

            @pl.loop(t + AHEAD - last * (AHEAD - 1), t + AHEAD + 1)
            def _(u):
                row_sends(u)

        @pl.when(jnp.logical_and(t >= Y_LAG, t < units + Y_LAG))
        def _():
            y_step(t - Y_LAG)

        @pl.when(jnp.logical_and(t >= 12, lax.rem(t, 4) == 0))
        def _():
            z_step(lax.div(t, 4) - 3)

    for slot in range(SLOTS):
        wait_sends(slot)
    gone = sent.at[:, pl.ds(0, (rows - 1) * chunks)]
    pltpu.make_async_copy(gone, gone, row_send).wait()


def solution(mesh):
    rows, cols = mesh.shape["row"], mesh.shape["col"]

    def local(velocity, symbol_x, symbol_y, symbol_z):
        nx, yl, zs = velocity.shape
        chunks, ny, nz = nx // rows, yl * rows, zs * cols
        ys, quarters = ny // cols, zs // LANES
        units = chunks * quarters
        table = jnp.asarray(stacked_table(nx))
        factors = [jnp.asarray(t) for t in factor_tables(nz)]
        anywhere = pl.BlockSpec(memory_space=pl.ANY)
        vmem = pl.BlockSpec(memory_space=pltpu.VMEM)
        dma = pltpu.SemaphoreType.DMA
        out, _ = pl.pallas_call(
            functools.partial(kernel, rows, cols),
            in_specs=[anywhere] + [vmem] * 5 + [pl.BlockSpec(memory_space=pltpu.SMEM), vmem, vmem],
            out_specs=(vmem, anywhere),
            out_shape=(
                pltpu.VMEM((chunks, ys, nz), F32),
                jax.ShapeDtypeStruct((quarters, nx, yl, LANES), F32),
            ),
            scratch_shapes=[
                pltpu.VMEM((units, ny, LANES), F32),
                pltpu.VMEM((chunks, nz // LANES, ys, LANES), F32),
                pltpu.VMEM((nz // 2, nz), BF16),
                pltpu.VMEM((nz // 2, nz), BF16),
                pltpu.VMEM((SLOTS, ny, LANES), F32),
                pltpu.VMEM((3 * ny, LANES), BF16),
                pltpu.VMEM((4 * ys, nz // 2), BF16),
                pltpu.VMEM((ys, LANES), F32),
                dma((2,)), dma((2,)), dma, dma((units,)), dma((units,)), dma((SLOTS,)), dma((chunks,)),
                pltpu.SemaphoreType.REGULAR,
            ],
            compiler_params=pltpu.CompilerParams(collective_id=0, has_side_effects=True, vmem_limit_bytes=46 * 2**20),
        )(velocity, table, *factors, symbol_x, symbol_y[None, :], symbol_z[None, :])
        return out

    placed = (P(None, "row", "col"), P(), P(), P())
    return jax.shard_map(local, mesh=mesh, in_specs=placed, out_specs=P("row", "col", None), check_vma=False)
```

```python
import functools

import jax
import jax.numpy as jnp
import numpy as np
from jax import lax
from jax.experimental import pallas as pl
from jax.experimental.pallas import tpu as pltpu
from jax.sharding import PartitionSpec as P

MESH = pl.DeviceIdType.MESH
F32 = jnp.float32
BF16 = jnp.bfloat16
FINE = 32
LANES = 128
Y_BLOCK = 8
FIRST = 4
AHEAD = 4
Y_LAG = 3
SLOTS = 8


def split(values):
    head = values.astype(BF16)
    return head, (values - head.astype(F32)).astype(BF16)


def mode_table(count):
    rank = np.arange(count)
    angle = 2.0 * np.pi / count * (rank[:, None] * rank[None, :] % count)
    return ((np.cos(angle) + np.sin(angle)) / np.sqrt(count)).astype(np.float32)


def stacked_table(count):
    table = mode_table(count)
    head = table.astype(BF16)
    rest = (table - head.astype(np.float32)).astype(BF16)
    return np.concatenate([head, rest, head], axis=1)


def factor_tables(count):
    k = np.arange(count)
    coarse = 2.0 * np.pi / count * (FINE * np.arange(count // 2 // FINE)[:, None] * k % count)
    fine = 2.0 * np.pi / count * (np.arange(FINE)[:, None] * k % count)
    scale = 1.0 / np.sqrt(count)
    tables = np.cos(coarse), np.sin(coarse), (np.cos(fine) + np.sin(fine)) * scale, (np.cos(fine) - np.sin(fine)) * scale
    return [t.astype(np.float32) for t in tables]


def kernel(
    rows, cols, velocity, h_ref, cos_ref, sin_ref, plus_ref, minus_ref, sx_ref, sy_ref, sz_ref, out, sent,
    got_y, got_z, t_head, t_rest, made_y, parts_y, parts_z, sy_col,
    in_sem, keep_sem, row_send, row_recv, own_sem, col_send, col_recv, free_sem,
):
    nx, yl, zs = velocity.shape
    chunks, ys, nz = out.shape
    ny = yl * rows
    quarters = zs // LANES
    units = chunks * quarters
    halves = yl // Y_BLOCK
    blocks = quarters * halves
    early = FIRST * quarters
    row, col = lax.axis_index("row"), lax.axis_index("col")
    mine = pl.ds(pl.multiple_of(row * yl, yl), yl)

    ring_y = [lax.rem(lax.div(row, 8) + d, 4) * 8 for d in range(4)]
    ring_x = [lax.rem(lax.div(row, 2) + d, 4) * 2 for d in range(4)]
    pair = [lax.rem(row + d, 2) for d in range(2)]
    far = sorted(range(1, rows), key=lambda o: -(min(o // 8, 4 - o // 8) + min(o // 2 % 4, 4 - o // 2 % 4)))
    peers = [ring_y[o // 8] + ring_x[o // 2 % 4] + pair[o % 2] for o in far]

    def place(u):
        first = lax.div(units + early - 1 - u, units)
        j = first * lax.rem(u, FIRST) + (1 - first) * lax.div(u, quarters)
        q = first * lax.div(u, FIRST) + (1 - first) * lax.rem(u, quarters)
        return j, q

    def block_of(ref, b):
        y, z = lax.rem(b, halves), lax.div(b, halves)
        return ref.at[:, pl.ds(pl.multiple_of(y * Y_BLOCK, Y_BLOCK), Y_BLOCK), pl.ds(pl.multiple_of(z * LANES, LANES), LANES)]

    def kept_at(b):
        y, z = lax.rem(b, halves), lax.div(b, halves)
        return sent.at[z, :, pl.ds(pl.multiple_of(y * Y_BLOCK, Y_BLOCK), Y_BLOCK), :]

    late = chunks // 2
    tiles = got_z.reshape(chunks * nz * ys // LANES // Y_BLOCK, Y_BLOCK, LANES)
    lines = got_z.reshape(chunks * nz * ys // LANES, LANES)
    base = late * nz * ys // LANES // Y_BLOCK

    def load(b):
        slot = lax.rem(b, 2)
        at = pl.ds(base + slot * nx, nx)
        return pltpu.make_async_copy(block_of(velocity, b), tiles.at[at], in_sem.at[slot])

    def keep(b):
        slot = lax.rem(b, 2)
        at = pl.ds(base + (2 + slot) * nx, nx)
        return pltpu.make_async_copy(tiles.at[at], kept_at(b), keep_sem.at[slot])

    def x_step(b):
        slot = lax.rem(b, 2)
        load(b).wait()
        v = lines.at[pl.ds(pl.multiple_of((base + slot * nx) * Y_BLOCK, Y_BLOCK), nx * Y_BLOCK)]
        o = lines.at[pl.ds(pl.multiple_of((base + (2 + slot) * nx) * Y_BLOCK, Y_BLOCK), nx * Y_BLOCK)]
        for y in range(0, Y_BLOCK, 2):
            for n in (y, y + 1):
                head, rest = split(v[pl.ds(n, nx, stride=Y_BLOCK), :])
                at = pl.ds(n * LANES, LANES)
                t_head[0:nx, at] = head
                t_head[nx : 2 * nx, at] = head
                t_rest[0:nx, at] = rest
            lanes = slice(y * LANES, (y + 2) * LANES)
            made = jnp.dot(h_ref[:, : 2 * nx], t_head[0 : 2 * nx, lanes], preferred_element_type=F32)
            made += jnp.dot(h_ref[:, 2 * nx :], t_rest[0:nx, lanes], preferred_element_type=F32)
            o[pl.ds(y, nx, stride=Y_BLOCK), :] = made[:, :LANES]
            o[pl.ds(y + 1, nx, stride=Y_BLOCK), :] = made[:, LANES:]
        keep(b).start()

        @pl.when(b + 2 < blocks)
        def _():
            load(b + 2).start()

    def own(u):
        j, q = place(u)
        return pltpu.make_async_copy(sent.at[q, row * chunks + j], got_y.at[u, mine], own_sem.at[u])

    def row_sends(u):
        j, q = place(u)

        to = got_y.at[u, mine]
        for p in peers:
            pltpu.make_async_remote_copy(
                src_ref=sent.at[q, p * chunks + j], dst_ref=to,
                send_sem=row_send, recv_sem=row_recv.at[u], device_id={"row": p}, device_id_type=MESH,
            ).start()

        own(u).start()

    def wait_sends(slot):
        sends = made_y.at[slot, pl.ds(0, (cols - 1) * ys)]
        pltpu.make_async_copy(sends, sends, col_send.at[slot]).wait()

    def y_step(u):
        slot = lax.rem(u, SLOTS)
        j, q = place(u)
        own(u).wait()
        landed = got_y.at[u, pl.ds(0, (rows - 1) * yl)]
        pltpu.make_async_copy(landed, landed, row_recv.at[u]).wait()
        head, rest = split(got_y[u])
        parts_y[0:ny, :] = head
        parts_y[ny : 2 * ny, :] = head
        parts_y[2 * ny : 3 * ny, :] = rest

        @pl.when(u >= SLOTS)
        def _():
            wait_sends(slot)

        @pl.when(u == late * quarters)
        def _():
            pl.semaphore_wait(free_sem, cols - 1)

        made_y[slot] = jnp.dot(h_ref[...], parts_y[...], preferred_element_type=F32)
        to = got_z.at[j, col * quarters + q]
        to[...] = made_y[slot, pl.ds(pl.multiple_of(col * ys, ys), ys), :]
        for d in (1, 3, 2):
            p = lax.rem(col + d, cols)
            pltpu.make_async_remote_copy(
                src_ref=made_y.at[slot, pl.ds(pl.multiple_of(p * ys, ys), ys)], dst_ref=to,
                send_sem=col_send.at[slot], recv_sem=col_recv.at[j], device_id={"col": p}, device_id_type=MESH,
            ).start()

    def z_step(j):
        landed = got_z.at[j, pl.ds(0, (cols - 1) * quarters)]
        pltpu.make_async_copy(landed, landed, col_recv.at[j]).wait()
        fold = cols * quarters // 2
        for k in range(fold):
            low, high = got_z[j, k], got_z[j, k + fold]
            at = pl.ds(k * LANES, LANES)
            for n, value in enumerate((low + high, low - high)):
                head, rest = split(value)
                parts_z[n * ys : (n + 1) * ys, at] = head
                parts_z[(n + 2) * ys : (n + 3) * ys, at] = rest

        part = sx_ref[row * chunks + j] + sy_col[...]
        even = lax.rem(lax.broadcasted_iota(jnp.int32, (ys, LANES), 1), 2) == 0

        @pl.loop(0, nz // 512)
        def _(n):
            at = pl.ds(pl.multiple_of(n * 512, 512), 512)
            both = jnp.dot(parts_z[...], t_head[:, at], preferred_element_type=F32)
            small = jnp.dot(parts_z[0 : 2 * ys, :], t_rest[:, at], preferred_element_type=F32)
            total = both[: 2 * ys] + (both[2 * ys :] + small)
            for m in range(512 // LANES):
                lanes = slice(m * LANES, (m + 1) * LANES)
                value = jnp.where(even, total[:ys, lanes], total[ys:, lanes])
                to = pl.ds(pl.multiple_of(n * 512 + m * LANES, LANES), LANES)
                symbol = part + sz_ref[:, to]
                out[j, :, to] = value * ((1.0 - 0.2 * symbol) / (1.0 + 0.2 * symbol))

    load(0).start()
    load(1).start()
    barrier = pltpu.get_barrier_semaphore()

    @pl.loop(1, rows)
    def _(o):
        pl.semaphore_signal(barrier, inc=1, device_id={"row": lax.rem(row + o, rows)}, device_id_type=MESH)

    for d in range(1, cols):
        pl.semaphore_signal(barrier, inc=1, device_id={"col": lax.rem(col + d, cols)}, device_id_type=MESH)

    @pl.loop(0, halves)
    def _(t):
        x_step(t)

    pl.semaphore_wait(barrier, rows + cols - 2)

    @pl.loop(halves - 1, 4 * chunks + 9)
    def _(t):
        @pl.when(jnp.logical_and(t >= halves, t < blocks))
        def _():
            x_step(t)

        @pl.when(t < blocks)
        def _():
            @pl.when(lax.rem(t, halves) == halves - 1)
            def _():
                for h in range(halves):
                    keep(t - (halves - 1) + h).wait()

                ready = lax.div(t, halves) * FIRST

                @pl.loop(ready, ready + FIRST)
                def _(u):
                    row_sends(u)

                @pl.when(t == blocks - 1)
                def _():
                    for d in range(1, cols):
                        p = lax.rem(col + d, cols)
                        pl.semaphore_signal(free_sem, inc=1, device_id={"col": p}, device_id_type=MESH)

        @pl.when(jnp.logical_and(t >= early - AHEAD, t < units - AHEAD))
        def _():
            row_sends(t + AHEAD)

        @pl.when(jnp.logical_and(t >= Y_LAG, t < units + Y_LAG))
        def _():
            y_step(t - Y_LAG)

        @pl.when(jnp.logical_and(t >= blocks + 1, t < blocks + 9))
        def _():
            share = nz // 2 // FINE // 8
            start = (t - blocks - 1) * share

            @pl.loop(start, start + share)
            def _(i):
                table = cos_ref[pl.ds(i, 1), :] * plus_ref[...] + sin_ref[pl.ds(i, 1), :] * minus_ref[...]
                head, rest = split(table)
                at = pl.ds(pl.multiple_of(i * FINE, FINE), FINE)
                t_head[at, :] = head
                t_rest[at, :] = rest

            spread = jnp.broadcast_to(sy_ref[:, pl.ds(pl.multiple_of(col * ys, ys), ys)], (LANES, ys))
            sy_col[...] = spread.T

        first = lax.div(128 + 25 - t, 128)
        often = jnp.logical_and(jnp.logical_and(t >= 18, t < 26), lax.rem(t, 2) == 0)

        @pl.when(jnp.logical_or(often, jnp.logical_and(t >= 28, lax.rem(t, 4) == 0)))
        def _():
            z_step(first * (lax.div(t, 2) - 9) + (1 - first) * (lax.div(t, 4) - 3))

    for slot in range(SLOTS):
        wait_sends(slot)
    gone = sent.at[:, pl.ds(0, (rows - 1) * chunks)]
    pltpu.make_async_copy(gone, gone, row_send).wait()


def solution(mesh):
    rows, cols = mesh.shape["row"], mesh.shape["col"]

    def local(velocity, symbol_x, symbol_y, symbol_z):
        nx, yl, zs = velocity.shape
        chunks, ny, nz = nx // rows, yl * rows, zs * cols
        ys, quarters = ny // cols, zs // LANES
        units = chunks * quarters
        table = jnp.asarray(stacked_table(nx))
        factors = [jnp.asarray(t) for t in factor_tables(nz)]
        anywhere = pl.BlockSpec(memory_space=pl.ANY)
        vmem = pl.BlockSpec(memory_space=pltpu.VMEM)
        dma = pltpu.SemaphoreType.DMA
        out, _ = pl.pallas_call(
            functools.partial(kernel, rows, cols),
            in_specs=[anywhere] + [vmem] * 5 + [pl.BlockSpec(memory_space=pltpu.SMEM), vmem, vmem],
            out_specs=(vmem, anywhere),
            out_shape=(
                pltpu.VMEM((chunks, ys, nz), F32),
                jax.ShapeDtypeStruct((quarters, nx, yl, LANES), F32),
            ),
            scratch_shapes=[
                pltpu.VMEM((units, ny, LANES), F32),
                pltpu.VMEM((chunks, nz // LANES, ys, LANES), F32),
                pltpu.VMEM((nz // 2, nz), BF16),
                pltpu.VMEM((nz // 2, nz), BF16),
                pltpu.VMEM((SLOTS, ny, LANES), F32),
                pltpu.VMEM((3 * ny, LANES), BF16),
                pltpu.VMEM((4 * ys, nz // 2), BF16),
                pltpu.VMEM((ys, LANES), F32),
                dma((2,)), dma((2,)), dma, dma((units,)), dma((units,)), dma((SLOTS,)), dma((chunks,)),
                pltpu.SemaphoreType.REGULAR,
            ],
            compiler_params=pltpu.CompilerParams(collective_id=0, has_side_effects=True, vmem_limit_bytes=47 * 2**20),
        )(velocity, table, *factors, symbol_x, symbol_y[None, :], symbol_z[None, :])
        return out

    placed = (P(None, "row", "col"), P(), P(), P())
    return jax.shard_map(local, mesh=mesh, in_specs=placed, out_specs=P("row", "col", None), check_vma=False)
```
